64 devices in a mesh: rep: 4 (over x, y), dp: 16 (over z, core).
Axes of the slice: x: 2, y: 2, z: 8, core: 2. Of those that a mesh axis runs over, the one named last changes fastest.
The devices are a block of a 4x4x8 slice.
Arguments:
- x: bfloat16 [64, 1024, 640], P(('rep', 'dp')), parts along dimension 0
- dy: bfloat16 [64, 1024, 640], P(('rep', 'dp')), parts along dimension 0
- w_gate: bfloat16 [2, 640, 4096], replicated
- w_up: bfloat16 [2, 640, 4096], replicated
- w_down: bfloat16 [2, 4096, 640], replicated
- m_w_gate: float32 [2, 640, 4096], replicated
- m_w_up: float32 [2, 640, 4096], replicated
- m_w_down: float32 [2, 4096, 640], replicated
- v_w_gate: float32 [2, 640, 4096], replicated
- v_w_up: float32 [2, 640, 4096], replicated
- v_w_down: float32 [2, 4096, 640], replicated
Outputs:
- output 1: bfloat16 [8, 640, 4096], P('rep'), parts along dimension 0
- output 2: bfloat16 [8, 640, 4096], P('rep'), parts along dimension 0
- output 3: bfloat16 [8, 4096, 640], P('rep'), parts along dimension 0
- output 4: float32 [8, 640, 4096], P('rep'), parts along dimension 0
- output 5: float32 [8, 640, 4096], P('rep'), parts along dimension 0
- output 6: float32 [8, 4096, 640], P('rep'), parts along dimension 0
- output 7: float32 [8, 640, 4096], P('rep'), parts along dimension 0
- output 8: float32 [8, 640, 4096], P('rep'), parts along dimension 0
- output 9: float32 [8, 4096, 640], P('rep'), parts along dimension 0
There are 4 independent parts. The reference program is written for one: setup_inputs(seed, part) draws one part's arguments, and reference() takes and returns one part's arrays. A program takes and returns all parts, laid end to end along the dimension named above; an argument that names none is the same for every part.
All inputs are finite; a program needn't handle non-finite values.
Results may differ from the reference program's by a relative error of at most 0.0226.
Values are sent between devices in bfloat16 or wider.
A program may use at most 768 MiB of HBM per device.

```python
import jax
import jax.numpy as jnp
from jax import lax

SEQUENCES = 16
TOKENS = 1024
D = 640
FF = 4096
LAYERS = 2
NAMES = ("w_gate", "w_up", "w_down")
SHAPES = {"w_gate": (LAYERS, D, FF), "w_up": (LAYERS, D, FF), "w_down": (LAYERS, FF, D)}


def bump(key, n, height):
    away = (jnp.arange(n, dtype=jnp.int32) - jax.random.randint(key, (), 0, n, jnp.int32)) % n
    return jnp.where(away < n // 8, height, 1.0)


def together(key, own, strength):
    shared = jax.random.normal(key, own.shape[1:], jnp.float32)
    return (own + strength * shared) * lax.rsqrt(1 + strength * strength)


def setup_inputs(seed: int = 0, part: int = 0) -> dict:
    kx, kdy, ka, kb, kz, kf, kh, kl, *keys = jax.random.split(jax.random.key(seed), 8 + 3 * len(NAMES))
    kx, kdy, ka, kb = (jax.random.fold_in(k, part) for k in (kx, kdy, ka, kb))
    kw, km, kv = (keys[i::3] for i in range(3))
    shape = (SEQUENCES, TOKENS, D)
    much_x, much_dy = jax.random.uniform(kz, (2,), jnp.float32, 0.0, 1.0)
    loud = 2.0 ** jax.random.uniform(jax.random.fold_in(kz, 1), (), jnp.float32, -1.0, 2.0)
    layers = 2.0 ** jax.random.uniform(kl, (LAYERS, 1, 1), jnp.float32, -1.0, 1.0)
    x = together(ka, jax.random.normal(kx, shape, jnp.float32), much_x) * bump(kf, D, 4.0)
    dy = together(kb, jax.random.normal(kdy, shape, jnp.float32), much_dy)
    drawn = {"x": x.astype(jnp.bfloat16), "dy": (loud * dy * (SEQUENCES * TOKENS) ** -0.5).astype(jnp.bfloat16)}
    for key, name in zip(kw, NAMES, strict=True):
        w = jax.random.normal(key, SHAPES[name], jnp.float32) * SHAPES[name][1] ** -0.5
        drawn[name] = (w * {"w_gate": 1.0, "w_up": bump(kh, FF, 4.0), "w_down": layers}[name]).astype(jnp.bfloat16)
    for key, name in zip(km, NAMES, strict=True):
        drawn[f"m_{name}"] = 0.1 * jax.random.normal(key, SHAPES[name], jnp.float32)
    for key, name in zip(kv, NAMES, strict=True):
        drawn[f"v_{name}"] = jax.random.uniform(key, SHAPES[name], jnp.float32, 0.005, 0.015)
    return drawn


def matmul(a, w):
    return jnp.dot(a, w, preferred_element_type=jnp.float32).astype(jnp.bfloat16)


def normed(h):
    wide = h.astype(jnp.float32)
    scale = lax.rsqrt(jnp.mean(wide**2, -1, keepdims=True) + 1e-6)
    return (wide * scale).astype(jnp.bfloat16)


def layer(h, w):
    a = normed(h)
    gate = jnp.dot(a, w["w_gate"], preferred_element_type=jnp.float32)
    up = jnp.dot(a, w["w_up"], preferred_element_type=jnp.float32)
    return h + matmul((jax.nn.silu(gate) * up).astype(jnp.bfloat16), w["w_down"])


def adamw(w, m, v, g):
    m = 0.9 * m + 0.1 * g
    v = 0.95 * v + 0.05 * g * g
    step = m * lax.rsqrt(v + 1e-8) + 0.1 * w
    return (w - 0.02 * step).astype(jnp.bfloat16), m, v


def stack(weights, h):
    return lax.scan(lambda h, w: (layer(h, w), None), h, weights)[0]


def reference(x, dy, w_gate, w_up, w_down, m_w_gate, m_w_up, m_w_down, v_w_gate, v_w_up, v_w_down):
    weights = dict(zip(NAMES, (w_gate, w_up, w_down), strict=True))

    def take(so_far, sequence):
        h, by_y = sequence
        _, back = jax.vjp(lambda w: stack(w, h), weights)
        return jax.tree.map(lambda total, term: total + term.astype(jnp.float32), so_far, back(by_y)[0]), None

    none_yet = {name: jnp.zeros(w.shape, jnp.float32) for name, w in weights.items()}
    by_weights, _ = lax.scan(take, none_yet, (x, dy))
    gradients = [by_weights[name].astype(jnp.bfloat16).astype(jnp.float32) for name in NAMES]
    new = [
        adamw(w.astype(jnp.float32), m, v, g)
        for w, m, v, g in zip((w_gate, w_up, w_down), (m_w_gate, m_w_up, m_w_down), (v_w_gate, v_w_up, v_w_down), gradients, strict=True)
    ]
    return tuple(one[which] for which in range(3) for one in new)
```

```python
import functools

import jax
import jax.numpy as jnp
from jax import lax
from jax.experimental import pallas as pl
from jax.experimental.pallas import tpu as pltpu
from jax.sharding import PartitionSpec as P

MESH = pl.DeviceIdType.MESH
BF, F32 = jnp.bfloat16, jnp.float32
LANES = 128
TILE = 512
NS, NP, NR = 6, 6, 8
STEPS, STRIDE = 9, 5


def mm(a, b, ca, cb):
    return lax.dot_general(a, b, (((ca,), (cb,)), ((), ())), preferred_element_type=F32)


class Ring:
    def __init__(self, n):
        me = lax.axis_index("dp")
        self.Z = Z = n // 2
        self.z, self.c = z, c = lax.div(me, 2), lax.rem(me, 2)
        ahead = 2 * c - 1
        self.next = 2 * lax.rem(z + ahead + Z, Z) + c
        self.prev = 2 * lax.rem(z - ahead + Z, Z) + c
        self.mate = 2 * z + 1 - c
        down = lax.rem(Z - z, Z)
        self.p = jnp.where(c == 1, z, down)
        self.mate_p = jnp.where(c == 1, down, z)


def grads_kernel(n, layers, x_hbm, dy_hbm, wg_hbm, wu_hbm, wd_hbm, *refs):
    outs, refs = refs[:layers], refs[layers:]
    a, by, h, da, wg, wu, wd, hid, dgate, dup, full, pbuf, rs, in_sem, w_sem, d_send, d_recv, r_send, r_recv = refs
    at = Ring(n)
    Z, c, p = at.Z, at.c, at.p
    _, T, D = a.shape
    FF = wg_hbm.shape[2]
    NT = FF // TILE
    J = layers * NT
    F0 = (layers - 1) * NT
    HT = TILE // 2
    DR, FR = D // Z, HT // Z
    GC, DC = HT // LANES, D // LANES
    OFF_U, OFF_D = GC * DR, 2 * GC * DR
    RC = T // 4
    NB = min(256, TILE)

    def weights(t):
        l = jnp.where(t < F0, lax.div(t, NT), layers - 1 - lax.div(t - F0, NT))
        f, b = lax.rem(t, NT), lax.rem(t, 2)
        copies = []
        for x in range(2):
            src = pl.ds(pl.multiple_of(x * (FF // 2) + f * HT, HT), HT)
            dst = pl.ds(x * HT, HT)
            copies += [
                pltpu.make_async_copy(wg_hbm.at[l, :, src], wg.at[b, :, dst], w_sem.at[b, x, 0]),
                pltpu.make_async_copy(wu_hbm.at[l, :, src], wu.at[b, :, dst], w_sem.at[b, x, 1]),
                pltpu.make_async_copy(wd_hbm.at[l, src, :], wd.at[b, dst, :], w_sem.at[b, x, 2]),
            ]
        return copies

    def next_weights(t):
        for copy in weights(t):
            copy.wait()

        @pl.when(t + 1 < F0 + J)
        def _():
            for copy in weights(t + 1):
                copy.start()

    def by_rows(size, body):
        size = min(size, T)

        def block(k, _):
            body(pl.ds(pl.multiple_of(k * size, size), size))
            return 0

        lax.fori_loop(0, T // size, block, 0)

    def norm(l):
        def of(rows):
            wide = h[l, rows, :].astype(F32)
            a[l, rows, :] = (wide * lax.rsqrt(jnp.mean(wide * wide, -1, keepdims=True) + 1e-6)).astype(BF)

        by_rows(128, of)

    x_in = pltpu.make_async_copy(x_hbm.at[0], h.at[0], in_sem.at[0])
    dy_in = pltpu.make_async_copy(dy_hbm.at[0], by.at[layers - 1], in_sem.at[1])
    x_in.start()
    for copy in weights(0):
        copy.start()
    dy_in.start()
    bar = pltpu.get_barrier_semaphore()
    for other in (at.next, at.prev, at.mate):
        pl.semaphore_signal(bar, inc=1, device_id={"dp": other}, device_id_type=MESH)
    x_in.wait()
    norm(0)

    def forward(t, _):
        l, f, b = lax.div(t, NT), lax.rem(t, NT), lax.rem(t, 2)
        next_weights(t)

        @pl.when(f == 0)
        def _():
            da[...] = jnp.zeros_like(da)

        for w in range(4):
            rows = pl.ds(w * RC, RC)
            ar = a[l, rows, :]
            for nb in range(0, TILE, NB):
                cols = pl.ds(nb, NB)
                g = mm(ar, wg[b, :, cols], 1, 0)
                u = mm(ar, wu[b, :, cols], 1, 0)
                hid[rows, cols] = (g * u / (1 + jnp.exp(-g))).astype(BF)
            da[rows, :] += mm(hid[rows, :], wd[b], 1, 0)

        @pl.when(f == NT - 1)
        def _():
            def of(rows):
                h[l + 1, rows, :] = (h[l, rows, :].astype(F32) + da[rows, :].astype(BF).astype(F32)).astype(BF)

            by_rows(128, of)
            norm(l + 1)

        return 0

    lax.fori_loop(0, F0, forward, 0)
    dy_in.wait()
    pl.semaphore_wait(bar, 3)

    def piece(i, w):
        t = i + F0
        l, f, b, slot = layers - 1 - lax.div(i, NT), lax.rem(i, NT), lax.rem(t, 2), lax.rem(i, NS)
        if w == 0:
            next_weights(t)
        if w < 4:
            rows = pl.ds(w * RC, RC)
            ar, br = a[l, rows, :], by[l, rows, :]
            for nb in range(0, TILE, NB):
                cols = pl.ds(nb, NB)
                g = mm(ar, wg[b, :, cols], 1, 0)
                u = mm(ar, wu[b, :, cols], 1, 0)
                d = mm(br, wd[b, cols, :], 1, 1).astype(BF).astype(F32)
                s = 1 / (1 + jnp.exp(-g))
                gs = g * s
                hid[rows, cols] = (gs * u).astype(BF)
                dup[rows, cols] = (d * gs).astype(BF)
                dgate[rows, cols] = (d * u * (s + gs * (1 - s))).astype(BF)
        elif w == 4:
            for x in range(2):
                r = mm(hid[:, x * HT : (x + 1) * HT], by[l], 0, 0).astype(BF)
                for q in range(Z):
                    for k in range(DC):
                        full[slot, x, q, OFF_D + k * FR : OFF_D + (k + 1) * FR, :] = r[q * FR : (q + 1) * FR, k * LANES : (k + 1) * LANES]
        elif w in (5, 6):
            src, off = (dgate, 0) if w == 5 else (dup, OFF_U)
            for x in range(2):
                r = mm(a[l], src[:, x * HT : (x + 1) * HT], 0, 0).astype(BF)
                for q in range(Z):
                    for k in range(GC):
                        full[slot, x, q, off + k * DR : off + (k + 1) * DR, :] = r[q * DR : (q + 1) * DR, k * LANES : (k + 1) * LANES]
        else:
            rows = pl.ds((w - 7) * (T // 2), T // 2)

            def by_a():
                return mm(dgate[rows, :], wg[b], 1, 1) + mm(dup[rows, :], wu[b], 1, 1)

            @pl.when((l > 0) & (f == 0))
            def _():
                da[rows, :] = by_a()

            @pl.when((l > 0) & (f > 0))
            def _():
                da[rows, :] += by_a()

            if w == 8:

                @pl.when((l > 0) & (f == NT - 1))
                def _():
                    def of(rows):
                        wide = h[l, rows, :].astype(F32)
                        ct = da[rows, :].astype(BF).astype(F32)
                        scale = lax.rsqrt(jnp.mean(wide * wide, -1, keepdims=True) + 1e-6)
                        by_scale = jnp.sum(ct * wide, -1, keepdims=True)
                        g = ct * scale - wide * (by_scale * (scale * scale * scale) * (1.0 / D))
                        by[l - 1, rows, :] = (by[l, rows, :].astype(F32) + g.astype(BF).astype(F32)).astype(BF)

                    by_rows(128, of)

    def hop(j, e):
        slot, pb, r = lax.rem(j, NS), lax.rem(j, NP), lax.rem(j, NR)
        swap = pltpu.make_async_remote_copy(
            src_ref=full.at[slot, 1 - c],
            dst_ref=pbuf.at[pb],
            send_sem=d_send.at[pb],
            recv_sem=d_recv.at[pb],
            device_id={"dp": at.mate},
            device_id_type=MESH,
        )

        def ring(s):
            return pltpu.make_async_remote_copy(
                src_ref=rs.at[r, s],
                dst_ref=rs.at[r, s + 1],
                send_sem=r_send.at[r],
                recv_sem=r_recv.at[r, s + 1],
                device_id={"dp": at.next},
                device_id_type=MESH,
            )

        if e == 0:
            swap.start()
            return
        s = e - 1
        if s == 0:
            swap.wait_recv()
            swap.wait_send()
        else:
            last = ring(s - 1)
            last.wait_recv()
            last.wait_send()
        q = lax.rem(p + (2 * Z - 1 - s), Z)
        total = full[slot, c, q].astype(F32) + pbuf[pb, q].astype(F32)
        if s > 0:
            total = total + rs[r, s].astype(F32)
        if s < Z - 1:
            rs[r, s] = total.astype(BF)
            ring(s).start()
        else:
            for k, out in enumerate(outs):

                @pl.when(lax.div(j, NT) == k)
                def _():
                    out[lax.rem(j, NT)] = total.astype(BF)

    def macro(i, _):
        for w in range(STEPS):

            @pl.when(i < J)
            def _():
                piece(i, w)

            k = w % STRIDE
            j = i - 1 - k

            @pl.when((j >= 0) & (j < J))
            def _():
                hop(j, 2 * k + w // STRIDE)

        return 0

    lax.fori_loop(0, J + STRIDE, macro, 0)


def grads(n, x, dy, wg, wu, wd):
    layers, D, FF = wg.shape
    T = x.shape[1]
    Z, HT, NT = n // 2, TILE // 2, FF // TILE
    R = (2 * HT // LANES) * (D // Z) + (D // LANES) * (HT // Z)
    dma, vmem, anywhere = pltpu.SemaphoreType.DMA, pltpu.VMEM, pl.BlockSpec(memory_space=pl.ANY)
    return pl.pallas_call(
        functools.partial(grads_kernel, n, layers),
        out_shape=[jax.ShapeDtypeStruct((NT, R, LANES), BF)] * layers,
        in_specs=[anywhere] * 5,
        out_specs=[pl.BlockSpec(memory_space=pltpu.VMEM)] * layers,
        scratch_shapes=[
            vmem((layers, T, D), BF),
            vmem((layers, T, D), BF),
            vmem((layers, T, D), BF),
            vmem((T, D), F32),
            vmem((2, D, TILE), BF),
            vmem((2, D, TILE), BF),
            vmem((2, TILE, D), BF),
            vmem((T, TILE), BF),
            vmem((T, TILE), BF),
            vmem((T, TILE), BF),
            vmem((NS, 2, Z, R, LANES), BF),
            vmem((NP, Z, R, LANES), BF),
            vmem((NR, Z, R, LANES), BF),
            dma((2,)),
            dma((2, 2, 3)),
            dma((NP,)),
            dma((NP,)),
            dma((NR,)),
            dma((NR, Z)),
        ],
        compiler_params=pltpu.CompilerParams(collective_id=0, has_side_effects=True, vmem_limit_bytes=63 << 20),
        cost_estimate=pl.CostEstimate(flops=2 * T * D * FF * (11 * layers - 5), bytes_accessed=64 << 20, transcendentals=0),
        name="grads",
    )(x, dy, wg, wu, wd)


def adamw(w, m, v, g):
    m = 0.9 * m + 0.1 * g
    v = 0.95 * v + 0.05 * g * g
    step = m * lax.rsqrt(v + 1e-8) + 0.1 * w
    return (w - 0.02 * step).astype(BF), m, v


def update_kernel(n, l, s, again, *refs):
    (mine, mates), refs = refs[:2], refs[2:]
    olds, refs = refs[:9], refs[9 * (2 if again else 1) :]
    news, done, (g, *bufs), (g_sem, in_sem, out_sem) = refs[:9], refs[9], refs[10:20], refs[20:]
    at = Ring(n)
    Z = at.Z
    NT, R, _ = mine.shape
    D, FF = olds[0].shape[1:]
    HT = TILE // 2
    DR, FR = D // Z, HT // Z
    GC, DC = HT // LANES, D // LANES
    half_nt = NT // 2
    CW = half_nt * HT

    def place(arrays, unit):
        side, part = lax.div(unit, 2), lax.rem(unit, 2)
        q = lax.rem(jnp.where(side == 0, at.p, at.mate_p) + (Z - s), Z)
        half = jnp.where(side == 0, at.c, 1 - at.c)
        rows = pl.ds(pl.multiple_of(q * DR, DR), DR)
        cols = pl.ds(pl.multiple_of(half * (FF // 2) + part * CW, CW), CW)
        return [x.at[l, rows, cols] for x in arrays[:6]] + [x.at[l, half, pl.ds(part * half_nt, half_nt), q] for x in arrays[6:]]

    def loads(unit):
        return [pltpu.make_async_copy(src, buf.at[unit], in_sem.at[unit, k]) for k, (src, buf) in enumerate(zip(place(olds, unit), bufs, strict=True))]

    def stores(unit):
        return [pltpu.make_async_copy(buf.at[unit], dst, out_sem.at[unit, k]) for k, (dst, buf) in enumerate(zip(place(news, unit), bufs, strict=True))]

    terms = [pltpu.make_async_copy(src, g.at[k], g_sem.at[k]) for k, src in enumerate((mine, mates))]
    for copy in terms:
        copy.start()
    for unit in range(4):
        for copy in loads(unit):
            copy.start()
    for copy in terms:
        copy.wait()

    def one(unit, _):
        for copy in loads(unit):
            copy.wait()
        side, part = lax.div(unit, 2), lax.rem(unit, 2)

        def tile(t, _):
            def step(which, block, index):
                grad = g[side, part * half_nt + t, block, :].astype(F32)
                w, m, v = (bufs[3 * which + k] for k in range(3))
                w[index], m[index], v[index] = adamw(w[index].astype(F32), m[index], v[index], grad)

            for which in range(2):
                for k in range(GC):
                    cols = pl.ds(pl.multiple_of(t * HT + k * LANES, LANES), LANES)
                    step(which, pl.ds((which * GC + k) * DR, DR), (unit, slice(None), cols))
            for k in range(DC):
                step(2, pl.ds(2 * GC * DR + k * FR, FR), (unit, t, slice(None), pl.ds(k * LANES, LANES)))
            return 0

        lax.fori_loop(0, half_nt, tile, 0)
        for copy in stores(unit):
            copy.start()
        return 0

    lax.fori_loop(0, 4, one, 0)

    def end(unit, _):
        for copy in stores(unit):
            copy.wait()
        return 0

    lax.fori_loop(0, 4, end, 0)
    done[...] = jnp.zeros_like(done)


def update(n, l, s, mine, mates, olds, news):
    NT, R, _ = mine.shape
    D, FF = olds[0].shape[1:]
    Z = n // 2
    dma, vmem, anywhere = pltpu.SemaphoreType.DMA, pltpu.VMEM, pl.BlockSpec(memory_space=pl.ANY)
    again = news is not None
    wide, tall = (4, D // Z, FF // 4), (4, NT // 2, TILE // 2 // Z, D)
    types = [BF, F32, F32]
    return pl.pallas_call(
        functools.partial(update_kernel, n, l, s, again),
        out_shape=[jax.ShapeDtypeStruct(x.shape, x.dtype) for x in olds] + [jax.ShapeDtypeStruct((8, LANES), F32)],
        in_specs=[anywhere] * (2 + 9 * (2 if again else 1)),
        out_specs=[anywhere] * 9 + [pl.BlockSpec(memory_space=pltpu.VMEM)],
        input_output_aliases={11 + k: k for k in range(9)} if again else {},
        scratch_shapes=[vmem((2, NT, R, LANES), BF)]
        + [vmem(wide, t) for t in types] * 2
        + [vmem(tall, t) for t in types]
        + [dma((2,)), dma((4, 9)), dma((4, 9))],
        compiler_params=pltpu.CompilerParams(vmem_limit_bytes=63 << 20),
        cost_estimate=pl.CostEstimate(flops=8 * 10**9, bytes_accessed=22 * mine.size * 2, transcendentals=mine.size * 2),
        name="update",
    )(mine, mates, *olds, *(news or ()))


def solution(mesh):
    n = mesh.shape["dp"]
    Z = n // 2
    onward = [(2 * z + c, 2 * ((z + 2 * c - 1) % Z) + c) for z in range(Z) for c in range(2)]
    across = [(2 * z + c, 2 * z + 1 - c) for z in range(Z) for c in range(2)]

    def step(x, dy, *arrays):
        weights, m, v = (arrays[i : i + 3] for i in (0, 3, 6))
        layers, D, FF = weights[0].shape
        NT = FF // TILE
        HT = TILE // 2
        terms = list(grads(n, x, dy, *weights))
        split = (layers, 2, NT, Z, HT // Z, D)
        olds = [y for w in range(3) for y in (weights[w], m[w], v[w])]
        shapes = [y.shape for y in olds]
        olds = olds[:6] + [y.reshape(split) for y in olds[6:]]
        news, mates = None, [lax.ppermute(term, "dp", across) for term in terms]
        ahead = [lax.ppermute(term, "dp", onward) for term in terms]
        for s in range(Z):
            for k in range(layers):
                *news, done = update(n, layers - 1 - k, s, terms[k], mates[k], olds, news)
                if s < Z - 1:
                    terms[k], _ = lax.optimization_barrier((ahead[k], done))
                    if s < Z - 2:
                        ahead[k] = lax.ppermute(terms[k], "dp", onward)
                    mates[k] = lax.ppermute(terms[k], "dp", across)
        news = [y.reshape(shape) for y, shape in zip(news, shapes, strict=True)]
        return tuple(news[3 * w + which] for which in range(3) for w in range(3))

    return jax.shard_map(
        step,
        mesh=mesh,
        in_specs=(P(("rep", "dp"), None, None),) * 2 + (P(None, None, None),) * 9,
        out_specs=(P("rep", None, None),) * 9,
        check_vma=False,
    )
```

```python
import functools

import jax
import jax.numpy as jnp
from jax import lax
from jax.experimental import pallas as pl
from jax.experimental.pallas import tpu as pltpu
from jax.sharding import PartitionSpec as P


MESH = pl.DeviceIdType.MESH
BF, F32 = jnp.bfloat16, jnp.float32
LANES = 128
TILE = 512
NS, NP, NR = 5, 5, 5
STEPS, STRIDE, LAG = 9, 6, 3
PARTS, AHEAD = 2, 4


def mm(a, b, ca, cb):
    return lax.dot_general(a, b, (((ca,), (cb,)), ((), ())), preferred_element_type=F32)


class Ring:
    def __init__(self, n):
        me = lax.axis_index("dp")
        self.Z = Z = n // 2
        self.z, self.c = z, c = lax.div(me, 2), lax.rem(me, 2)
        ahead = 2 * c - 1
        self.next = 2 * lax.rem(z + ahead + Z, Z) + c
        self.prev = 2 * lax.rem(z - ahead + Z, Z) + c
        self.mate = 2 * z + 1 - c
        down = lax.rem(Z - z, Z)
        self.p = jnp.where(c == 1, z, down)
        self.mate_p = jnp.where(c == 1, down, z)


def grads_kernel(n, layers, x_hbm, dy_hbm, wg_hbm, wu_hbm, wd_hbm, *refs):
    outs, refs = refs[:layers], refs[layers:]
    a, by, h, da, wg, wu, wd, hid, dgate, dup, full, pbuf, on, back, in_sem, w_sem, d_send, d_recv, on_send, on_recv, back_send, back_recv = refs
    at = Ring(n)
    Z, c, p = at.Z, at.c, at.p
    _, T, D = a.shape
    FF = wg_hbm.shape[2]
    NT = FF // TILE
    J = layers * NT
    F0 = (layers - 1) * NT
    HT = TILE // 2
    DR, FR = D // Z, HT // Z
    GC, DC = HT // LANES, D // LANES
    OFF_U, OFF_D = GC * DR, 2 * GC * DR
    RC = T // 4
    NB = min(256, TILE)
    UP = Z // 2
    DOWN = Z - 1 - UP

    def weights(t):
        l = jnp.where(t < F0, lax.div(t, NT), layers - 1 - lax.div(t - F0, NT))
        f, b = lax.rem(t, NT), lax.rem(t, 2)
        copies = []
        for x in range(2):
            src = pl.ds(pl.multiple_of(x * (FF // 2) + f * HT, HT), HT)
            dst = pl.ds(x * HT, HT)
            copies += [
                pltpu.make_async_copy(wg_hbm.at[l, :, src], wg.at[b, :, dst], w_sem.at[b, x, 0]),
                pltpu.make_async_copy(wu_hbm.at[l, :, src], wu.at[b, :, dst], w_sem.at[b, x, 1]),
                pltpu.make_async_copy(wd_hbm.at[l, src, :], wd.at[b, dst, :], w_sem.at[b, x, 2]),
            ]
        return copies

    def next_weights(t):
        for copy in weights(t):
            copy.wait()

        @pl.when(t + 1 < F0 + J)
        def _():
            for copy in weights(t + 1):
                copy.start()

    def by_rows(size, body):
        size = min(size, T)

        def block(k, _):
            body(pl.ds(pl.multiple_of(k * size, size), size))
            return 0

        lax.fori_loop(0, T // size, block, 0)

    def norm(l):
        def of(rows):
            wide = h[l, rows, :].astype(F32)
            a[l, rows, :] = (wide * lax.rsqrt(jnp.mean(wide * wide, -1, keepdims=True) + 1e-6)).astype(BF)

        by_rows(128, of)

    x_in = pltpu.make_async_copy(x_hbm.at[0], h.at[0], in_sem.at[0])
    dy_in = pltpu.make_async_copy(dy_hbm.at[0], by.at[layers - 1], in_sem.at[1])
    x_in.start()
    for copy in weights(0):
        copy.start()
    dy_in.start()
    bar = pltpu.get_barrier_semaphore()
    for other in (at.next, at.prev, at.mate):
        pl.semaphore_signal(bar, inc=1, device_id={"dp": other}, device_id_type=MESH)
    x_in.wait()
    norm(0)

    def forward(t, _):
        l, f, b = lax.div(t, NT), lax.rem(t, NT), lax.rem(t, 2)
        next_weights(t)

        @pl.when(f == 0)
        def _():
            da[...] = jnp.zeros_like(da)

        for w in range(4):
            rows = pl.ds(w * RC, RC)
            ar = a[l, rows, :]
            for nb in range(0, TILE, NB):
                cols = pl.ds(nb, NB)
                g = mm(ar, wg[b, :, cols], 1, 0)
                u = mm(ar, wu[b, :, cols], 1, 0)
                hid[rows, cols] = (g * (1 / (1 + jnp.exp(-g))) * u).astype(BF)
            da[rows, :] += mm(hid[rows, :], wd[b], 1, 0)

        @pl.when(f == NT - 1)
        def _():
            def of(rows):
                h[l + 1, rows, :] = (h[l, rows, :].astype(F32) + da[rows, :].astype(BF).astype(F32)).astype(BF)

            by_rows(128, of)
            norm(l + 1)

        return 0

    lax.fori_loop(0, F0, forward, 0)
    dy_in.wait()
    pl.semaphore_wait(bar, 3)

    def piece(i, w):
        t = i + F0
        l, f, b, slot = layers - 1 - lax.div(i, NT), lax.rem(i, NT), lax.rem(t, 2), lax.rem(i, NS)
        if w == 0:
            next_weights(t)
        if w < 4:
            rows = pl.ds(w * RC, RC)
            ar, br = a[l, rows, :], by[l, rows, :]
            for nb in range(0, TILE, NB):
                cols = pl.ds(nb, NB)
                g = mm(ar, wg[b, :, cols], 1, 0)
                u = mm(ar, wu[b, :, cols], 1, 0)
                d = mm(br, wd[b, cols, :], 1, 1).astype(BF).astype(F32)
                s = 1 / (1 + jnp.exp(-g))
                gs = g * s
                hid[rows, cols] = (gs * u).astype(BF)
                dup[rows, cols] = (d * gs).astype(BF)
                dgate[rows, cols] = (d * u * (s + gs * (1 - s))).astype(BF)
        elif w == 4:
            for x in range(2):
                r = mm(hid[:, x * HT : (x + 1) * HT], by[l], 0, 0).astype(BF)
                for q in range(Z):
                    for k in range(DC):
                        full[slot, x, q, OFF_D + k * FR : OFF_D + (k + 1) * FR, :] = r[q * FR : (q + 1) * FR, k * LANES : (k + 1) * LANES]
        elif w in (5, 6):
            src, off = (dgate, 0) if w == 5 else (dup, OFF_U)
            for x in range(2):
                r = mm(a[l], src[:, x * HT : (x + 1) * HT], 0, 0).astype(BF)
                for q in range(Z):
                    for k in range(GC):
                        full[slot, x, q, off + k * DR : off + (k + 1) * DR, :] = r[q * DR : (q + 1) * DR, k * LANES : (k + 1) * LANES]
        else:
            rows = pl.ds((w - 7) * (T // 2), T // 2)

            def by_a():
                return mm(dgate[rows, :], wg[b], 1, 1) + mm(dup[rows, :], wu[b], 1, 1)

            @pl.when((l > 0) & (f == 0))
            def _():
                da[rows, :] = by_a()

            @pl.when((l > 0) & (f > 0))
            def _():
                da[rows, :] += by_a()

            if w == 8:

                @pl.when((l > 0) & (f == NT - 1))
                def _():
                    def of(rows):
                        wide = h[l, rows, :].astype(F32)
                        ct = da[rows, :].astype(BF).astype(F32)
                        scale = lax.rsqrt(jnp.mean(wide * wide, -1, keepdims=True) + 1e-6)
                        by_scale = jnp.sum(ct * wide, -1, keepdims=True)
                        g = ct * scale - wide * (by_scale * (scale * scale * scale) * (1.0 / D))
                        by[l - 1, rows, :] = (by[l, rows, :].astype(F32) + g.astype(BF).astype(F32)).astype(BF)

                    by_rows(128, of)

    def event(j, what, s):
        slot, pb, r = lax.rem(j, NS), lax.rem(j, NP), lax.rem(j, NR)
        swap = pltpu.make_async_remote_copy(
            src_ref=full.at[slot, 1 - c],
            dst_ref=pbuf.at[pb],
            send_sem=d_send.at[pb],
            recv_sem=d_recv.at[pb],
            device_id={"dp": at.mate},
            device_id_type=MESH,
        )

        def send(sums, s, send_sem, recv_sem, to):
            return pltpu.make_async_remote_copy(
                src_ref=sums.at[r, s],
                dst_ref=sums.at[r, s + 1],
                send_sem=send_sem.at[r],
                recv_sem=recv_sem.at[r, s + 1],
                device_id={"dp": to},
                device_id_type=MESH,
            )

        onwards = lambda s: send(on, s, on_send, on_recv, at.next)
        backwards = lambda s: send(back, s, back_send, back_recv, at.prev)

        def own(q):
            q = lax.rem(q + 2 * Z, Z)
            return full[slot, c, q].astype(F32) + pbuf[pb, q].astype(F32)

        if what == "give":
            swap.start()
        elif what == "on":
            if s:
                onwards(s - 1).wait_recv()
                onwards(s - 1).wait_send()
            else:
                swap.wait_recv()
                swap.wait_send()
            total = own(p + UP - s)
            on[r, s] = (total + on[r, s].astype(F32) if s else total).astype(BF)
            onwards(s).start()
        elif what == "back":
            if s:
                backwards(s - 1).wait_recv()
                backwards(s - 1).wait_send()
            total = own(p - DOWN + s)
            back[r, s] = (total + back[r, s].astype(F32) if s else total).astype(BF)
            backwards(s).start()
        else:
            for copy in (onwards(UP - 1), backwards(DOWN - 1)):
                copy.wait_recv()
                copy.wait_send()
            total = (own(p) + on[r, UP].astype(F32) + back[r, DOWN].astype(F32)).astype(BF)
            for k, out in enumerate(outs):

                @pl.when(lax.div(j, NT) == k)
                def _():
                    out[lax.rem(j, NT)] = total

    events = [(0, "give", 0)] + [(STRIDE * (s + 1), "on", s) for s in range(UP)] + [(STRIDE * (s + 1) + LAG, "back", s) for s in range(DOWN)]
    events.append((STRIDE * (UP + 1), "end", 0))

    def macro(i, _):
        for w in range(STEPS):

            @pl.when(i < J)
            def _():
                piece(i, w)

            for wait, what, s in sorted(events, reverse=True):
                if wait % STEPS == w:
                    j = i - 1 - wait // STEPS

                    @pl.when((j >= 0) & (j < J))
                    def _():
                        event(j, what, s)

        return 0

    lax.fori_loop(0, J + 1 + max(events)[0] // STEPS, macro, 0)


def grads(n, x, dy, wg, wu, wd):
    layers, D, FF = wg.shape
    T = x.shape[1]
    Z, HT, NT = n // 2, TILE // 2, FF // TILE
    R = (2 * HT // LANES) * (D // Z) + (D // LANES) * (HT // Z)
    dma, vmem, anywhere = pltpu.SemaphoreType.DMA, pltpu.VMEM, pl.BlockSpec(memory_space=pl.ANY)
    return pl.pallas_call(
        functools.partial(grads_kernel, n, layers),
        out_shape=[jax.ShapeDtypeStruct((NT, R, LANES), BF)] * layers,
        in_specs=[anywhere] * 5,
        out_specs=[pl.BlockSpec(memory_space=pltpu.VMEM)] * layers,
        scratch_shapes=[
            vmem((layers, T, D), BF),
            vmem((layers, T, D), BF),
            vmem((layers, T, D), BF),
            vmem((T, D), F32),
            vmem((2, D, TILE), BF),
            vmem((2, D, TILE), BF),
            vmem((2, TILE, D), BF),
            vmem((T, TILE), BF),
            vmem((T, TILE), BF),
            vmem((T, TILE), BF),
            vmem((NS, 2, Z, R, LANES), BF),
            vmem((NP, Z, R, LANES), BF),
            vmem((NR, Z // 2 + 1, R, LANES), BF),
            vmem((NR, Z - Z // 2, R, LANES), BF),
            dma((2,)),
            dma((2, 2, 3)),
            dma((NP,)),
            dma((NP,)),
            dma((NR,)),
            dma((NR, Z // 2 + 1)),
            dma((NR,)),
            dma((NR, Z - Z // 2)),
        ],
        compiler_params=pltpu.CompilerParams(collective_id=0, has_side_effects=True, vmem_limit_bytes=53 << 20),
        cost_estimate=pl.CostEstimate(flops=2 * T * D * FF * (11 * layers - 5), bytes_accessed=64 << 20, transcendentals=0),
        name="grads",
    )(x, dy, wg, wu, wd)


def adamw(w, m, v, g):
    m = 0.9 * m + 0.1 * g
    v = 0.95 * v + 0.05 * g * g
    step = m * lax.rsqrt(v + 1e-8) + 0.1 * w
    return (w - 0.02 * step).astype(BF), m, v


def update_kernel(n, l, s, sides, unread, *refs):
    terms, refs = refs[: len(sides)], refs[len(sides) :]
    olds, refs = refs[:9], refs[9 + unread :]
    news, (g, *bufs), (g_sem, in_sem, out_sem) = refs[:9], refs[9:19], refs[19:]
    at = Ring(n)
    Z = at.Z
    NT, _, _ = terms[0].shape
    D, FF = olds[0].shape[1:]
    HT = TILE // 2
    DR, FR = D // Z, HT // Z
    GC, DC = HT // LANES, D // LANES
    units, tiles = len(sides) * PARTS, NT // PARTS
    CW = tiles * HT

    def place(arrays, unit):
        side, part = (lax.div(unit, PARTS) if len(sides) > 1 else sides[0]), lax.rem(unit, PARTS)
        q = lax.rem(jnp.where(side == 0, at.p, at.mate_p) + (Z - s), Z)
        half = jnp.where(side == 0, at.c, 1 - at.c)
        rows = pl.ds(pl.multiple_of(q * DR, DR), DR)
        cols = pl.ds(pl.multiple_of(half * (FF // 2) + part * CW, CW), CW)
        return [x.at[l, rows, cols] for x in arrays[:6]] + [x.at[l, half, pl.ds(part * tiles, tiles), q] for x in arrays[6:]]

    def loads(unit):
        return [pltpu.make_async_copy(src, buf.at[unit], in_sem.at[unit, k]) for k, (src, buf) in enumerate(zip(place(olds, unit), bufs, strict=True))]

    def stores(unit):
        return [pltpu.make_async_copy(buf.at[unit], dst, out_sem.at[unit, k]) for k, (dst, buf) in enumerate(zip(place(news, unit), bufs, strict=True))]

    fetched = [pltpu.make_async_copy(terms[0].at[k], g.at[k], g_sem.at[k]) for k in range(NT if 0 in sides else 0)]
    for unit in range(min(AHEAD, units)):
        for copy in (fetched[unit * tiles : (unit + 1) * tiles]) + loads(unit):
            copy.start()

    def one(unit, _):
        for k in range(len(fetched) // tiles):

            @pl.when(unit == k)
            def _():
                for copy in fetched[k * tiles : (k + 1) * tiles]:
                    copy.wait()

        for copy in loads(unit):
            copy.wait()

        @pl.when(unit + AHEAD < units)
        def _():
            for copy in loads(unit + AHEAD):
                copy.start()

        side, part = lax.div(unit, PARTS), lax.rem(unit, PARTS)

        def tile(t, _):
            def step(which, block, index):
                shards = [terms[k] if x else g for k, x in enumerate(sides)]
                grad = shards[0][part * tiles + t, block, :]
                if len(sides) > 1:
                    grad = jnp.where(side == 0, grad, shards[1][part * tiles + t, block, :])
                grad = grad.astype(F32)
                w, m, v = (bufs[3 * which + k] for k in range(3))
                w[index], m[index], v[index] = adamw(w[index].astype(F32), m[index], v[index], grad)

            for which in range(2):
                for k in range(GC):
                    cols = pl.ds(pl.multiple_of(t * HT + k * LANES, LANES), LANES)
                    step(which, pl.ds((which * GC + k) * DR, DR), (unit, slice(None), cols))
            for k in range(DC):
                step(2, pl.ds(2 * GC * DR + k * FR, FR), (unit, t, slice(None), pl.ds(k * LANES, LANES)))
            return 0

        lax.fori_loop(0, tiles, tile, 0)
        for copy in stores(unit):
            copy.start()
        return 0

    lax.fori_loop(0, units, one, 0)

    def end(unit, _):
        for copy in stores(unit):
            copy.wait()
        return 0

    lax.fori_loop(0, units, end, 0)


def update(n, l, s, terms, olds, news):
    sides, terms = tuple(terms), tuple(terms.values())
    NT, R, _ = terms[0].shape
    D, FF = olds[0].shape[1:]
    Z = n // 2
    dma, vmem, anywhere = pltpu.SemaphoreType.DMA, pltpu.VMEM, pl.BlockSpec(memory_space=pl.ANY)
    again = news is not None
    units, size = len(sides) * PARTS, len(sides) * terms[0].size
    wide, tall = (units, D // Z, FF // (2 * PARTS)), (units, NT // PARTS, TILE // 2 // Z, D)
    types = [BF, F32, F32]
    return pl.pallas_call(
        functools.partial(update_kernel, n, l, s, sides, 9 * again),
        out_shape=[jax.ShapeDtypeStruct(x.shape, x.dtype) for x in olds],
        in_specs=[pl.BlockSpec(memory_space=vmem) if x else anywhere for x in sides] + [anywhere] * (9 * (2 if again else 1)),
        out_specs=[anywhere] * 9,
        input_output_aliases={len(sides) + 9 + k: k for k in range(9)} if again else {},
        scratch_shapes=[vmem((NT, R, LANES), BF)]
        + [vmem(wide, t) for t in types] * 2
        + [vmem(tall, t) for t in types]
        + [dma((NT,)), dma((units, 9)), dma((units, 9))],
        compiler_params=pltpu.CompilerParams(vmem_limit_bytes=30 << 20),
        cost_estimate=pl.CostEstimate(flops=4 * 10**9 * len(sides), bytes_accessed=22 * size, transcendentals=size),
        name="update",
    )(*terms, *olds, *(news or ()))


def solution(mesh):
    n = mesh.shape["dp"]
    Z = n // 2
    onward = [(2 * z + c, 2 * ((z + 2 * c - 1) % Z) + c) for z in range(Z) for c in range(2)]
    across = [(2 * z + c, 2 * z + 1 - c) for z in range(Z) for c in range(2)]

    def step(x, dy, *arrays):
        weights, m, v = (arrays[i : i + 3] for i in (0, 3, 6))
        layers, D, FF = weights[0].shape
        NT = FF // TILE
        HT = TILE // 2
        terms = list(grads(n, x, dy, *weights))
        split = (layers, 2, NT, Z, HT // Z, D)
        olds = [y for w in range(3) for y in (weights[w], m[w], v[w])]
        shapes = [y.shape for y in olds]
        olds = olds[:6] + [y.reshape(split) for y in olds[6:]]

        def hop(k):
            return lax.ppermute(terms[k], "dp", onward)

        def swap(k):
            return lax.ppermute(terms[k], "dp", across)

        coming = [hop(k) for k in range(layers)]
        mates = [swap(k) for k in range(layers)]
        news = None
        for s in range(Z):
            for k in range(layers):
                shards = [{0: terms[k], 1: mates[k]}]
                if (k, s) == (layers - 1, Z - 1):
                    shards = [{0: terms[k]}, {1: mates[k]}]
                for part in shards:
                    news = update(n, layers - 1 - k, s, part, olds, news)
                if s < Z - 1:
                    terms[k] = coming[k]
                    if s < Z - 2:
                        coming[k] = hop(k)
                    mates[k] = swap(k)
        news = [y.reshape(shape) for y, shape in zip(news, shapes, strict=True)]
        return tuple(news[3 * w + which] for which in range(3) for w in range(3))

    return jax.shard_map(
        step,
        mesh=mesh,
        in_specs=(P(("rep", "dp"), None, None),) * 2 + (P(None, None, None),) * 9,
        out_specs=(P("rep", None, None),) * 9,
        check_vma=False,
    )
```

```python
import functools

import jax
import jax.numpy as jnp
from jax import lax
from jax.experimental import pallas as pl
from jax.experimental.pallas import tpu as pltpu
from jax.sharding import PartitionSpec as P


MESH = pl.DeviceIdType.MESH
BF, F32 = jnp.bfloat16, jnp.float32
LANES = 128
TILE = 512
NS, NP, NR = 5, 5, 5
STEPS, STRIDE, LAG = 9, 6, 3
GIVE = 9
PARTS, AHEAD = 2, 4


def mm(a, b, ca, cb):
    return lax.dot_general(a, b, (((ca,), (cb,)), ((), ())), preferred_element_type=F32)


class Ring:
    def __init__(self, n):
        me = lax.axis_index("dp")
        self.Z = Z = n // 2
        self.z, self.c = z, c = lax.div(me, 2), lax.rem(me, 2)
        ahead = 2 * c - 1
        self.next = 2 * lax.rem(z + ahead + Z, Z) + c
        self.prev = 2 * lax.rem(z - ahead + Z, Z) + c
        self.mate = 2 * z + 1 - c
        down = lax.rem(Z - z, Z)
        self.p = jnp.where(c == 1, z, down)
        self.mate_p = jnp.where(c == 1, down, z)


def grads_kernel(n, layers, x_hbm, dy_hbm, wg_hbm, wu_hbm, wd_hbm, *refs):
    outs, refs = refs[:layers], refs[layers:]
    a, by, h, da, wg, wu, wd, hid, dgate, dup, full, pbuf, on, back, in_sem, w_sem, d_send, d_recv, on_send, on_recv, back_send, back_recv = refs
    at = Ring(n)
    Z, c, p = at.Z, at.c, at.p
    _, T, D = a.shape
    FF = wg_hbm.shape[2]
    NT = FF // TILE
    J = layers * NT
    F0 = (layers - 1) * NT
    HT = TILE // 2
    DR, FR = D // Z, HT // Z
    GC, DC = HT // LANES, D // LANES
    OFF_U, OFF_D = GC * DR, 2 * GC * DR
    RC = T // 4
    NB = min(256, TILE)
    UP = Z // 2
    DOWN = Z - 1 - UP

    def weights(t):
        l = jnp.where(t < F0, lax.div(t, NT), layers - 1 - lax.div(t - F0, NT))
        f, b = lax.rem(t, NT), lax.rem(t, 2)
        copies = []
        for x in range(2):
            src = pl.ds(pl.multiple_of(x * (FF // 2) + f * HT, HT), HT)
            dst = pl.ds(x * HT, HT)
            copies += [
                pltpu.make_async_copy(wg_hbm.at[l, :, src], wg.at[b, :, dst], w_sem.at[b, x, 0]),
                pltpu.make_async_copy(wu_hbm.at[l, :, src], wu.at[b, :, dst], w_sem.at[b, x, 1]),
                pltpu.make_async_copy(wd_hbm.at[l, src, :], wd.at[b, dst, :], w_sem.at[b, x, 2]),
            ]
        return copies

    def next_weights(t):
        for copy in weights(t):
            copy.wait()

        @pl.when(t + 1 < F0 + J)
        def _():
            for copy in weights(t + 1):
                copy.start()

    def by_rows(size, body):
        size = min(size, T)

        def block(k, _):
            body(pl.ds(pl.multiple_of(k * size, size), size))
            return 0

        lax.fori_loop(0, T // size, block, 0)

    def normed(wide):
        return (wide * lax.rsqrt(jnp.mean(wide * wide, -1, keepdims=True) + 1e-6)).astype(BF)

    x_in = pltpu.make_async_copy(x_hbm.at[0], h.at[0], in_sem.at[0])
    dy_in = pltpu.make_async_copy(dy_hbm.at[0], by.at[layers - 1], in_sem.at[1])
    x_in.start()
    for copy in weights(0):
        copy.start()
    dy_in.start()
    bar = pltpu.get_barrier_semaphore()
    for other in (at.next, at.prev, at.mate):
        pl.semaphore_signal(bar, inc=1, device_id={"dp": other}, device_id_type=MESH)
    x_in.wait()

    def first(rows):
        a[0, rows, :] = normed(h[0, rows, :].astype(F32))

    by_rows(128, first)

    def forward(t, _):
        l, f, b = lax.div(t, NT), lax.rem(t, NT), lax.rem(t, 2)
        next_weights(t)

        @pl.when(f == 0)
        def _():
            da[...] = jnp.zeros_like(da)

        blocks = [(pl.ds(w * RC, RC), pl.ds(nb, NB)) for w in range(4) for nb in range(0, TILE, NB)]
        held = None
        for k in range(len(blocks) + 1):
            if k < len(blocks):
                rows, cols = blocks[k]
                ar = a[l, rows, :]
                g, u = mm(ar, wg[b, :, cols], 1, 0), mm(ar, wu[b, :, cols], 1, 0)
            if held is not None:
                g0, u0 = held
                rows0, cols0 = blocks[k - 1]
                hid[rows0, cols0] = (g0 * (1 / (1 + jnp.exp(-g0))) * u0).astype(BF)
                if k % (TILE // NB) == 0:
                    da[rows0, :] += mm(hid[rows0, :], wd[b], 1, 0)
            held = (g, u)

        @pl.when(f == NT - 1)
        def _():
            def of(rows):
                y = (h[l, rows, :].astype(F32) + da[rows, :].astype(BF).astype(F32)).astype(BF)
                h[l + 1, rows, :] = y
                a[l + 1, rows, :] = normed(y.astype(F32))

            by_rows(128, of)

        return 0

    lax.fori_loop(0, F0, forward, 0)
    dy_in.wait()
    pl.semaphore_wait(bar, 3)

    def piece(i, w):
        t = i + F0
        l, f, b, slot = layers - 1 - lax.div(i, NT), lax.rem(i, NT), lax.rem(t, 2), lax.rem(i, NS)
        if w == 0:
            next_weights(t)
        if w < 4:
            rows = pl.ds(w * RC, RC)
            ar, br = a[l, rows, :], by[l, rows, :]
            for nb in range(0, TILE, NB):
                cols = pl.ds(nb, NB)
                g = mm(ar, wg[b, :, cols], 1, 0)
                u = mm(ar, wu[b, :, cols], 1, 0)
                d = mm(br, wd[b, cols, :], 1, 1).astype(BF).astype(F32)
                s = 1 / (1 + jnp.exp(-g))
                gs = g * s
                hid[rows, cols] = (gs * u).astype(BF)
                dup[rows, cols] = (d * gs).astype(BF)
                dgate[rows, cols] = (d * u * (s + gs * (1 - s))).astype(BF)
        elif w == 4:
            for x in range(2):
                r = mm(hid[:, x * HT : (x + 1) * HT], by[l], 0, 0).astype(BF)
                for q in range(Z):
                    for k in range(DC):
                        full[slot, x, q, OFF_D + k * FR : OFF_D + (k + 1) * FR, :] = r[q * FR : (q + 1) * FR, k * LANES : (k + 1) * LANES]
        elif w in (5, 6):
            src, off = (dgate, 0) if w == 5 else (dup, OFF_U)
            for x in range(2):
                r = mm(a[l], src[:, x * HT : (x + 1) * HT], 0, 0).astype(BF)
                for q in range(Z):
                    for k in range(GC):
                        full[slot, x, q, off + k * DR : off + (k + 1) * DR, :] = r[q * DR : (q + 1) * DR, k * LANES : (k + 1) * LANES]
        else:
            rows = pl.ds((w - 7) * (T // 2), T // 2)

            def by_a():
                return mm(dgate[rows, :], wg[b], 1, 1) + mm(dup[rows, :], wu[b], 1, 1)

            @pl.when((l > 0) & (f == 0))
            def _():
                da[rows, :] = by_a()

            @pl.when((l > 0) & (f > 0))
            def _():
                da[rows, :] += by_a()

            if w == 8:

                @pl.when((l > 0) & (f == NT - 1))
                def _():
                    def of(rows):
                        wide = h[l, rows, :].astype(F32)
                        ct = da[rows, :].astype(BF).astype(F32)
                        scale = lax.rsqrt(jnp.mean(wide * wide, -1, keepdims=True) + 1e-6)
                        by_scale = jnp.sum(ct * wide, -1, keepdims=True)
                        g = ct * scale - wide * (by_scale * (scale * scale * scale) * (1.0 / D))
                        by[l - 1, rows, :] = (by[l, rows, :].astype(F32) + g.astype(BF).astype(F32)).astype(BF)

                    by_rows(128, of)

    def event(j, what, s):
        slot, pb, r = lax.rem(j, NS), lax.rem(j, NP), lax.rem(j, NR)
        swap = pltpu.make_async_remote_copy(
            src_ref=full.at[slot, 1 - c],
            dst_ref=pbuf.at[pb],
            send_sem=d_send.at[pb],
            recv_sem=d_recv.at[pb],
            device_id={"dp": at.mate},
            device_id_type=MESH,
        )

        def send(sums, s, send_sem, recv_sem, to):
            return pltpu.make_async_remote_copy(
                src_ref=sums.at[r, s],
                dst_ref=sums.at[r, s + 1],
                send_sem=send_sem.at[r],
                recv_sem=recv_sem.at[r, s + 1],
                device_id={"dp": to},
                device_id_type=MESH,
            )

        onwards = lambda s: send(on, s, on_send, on_recv, at.next)
        backwards = lambda s: send(back, s, back_send, back_recv, at.prev)

        def own(q):
            q = lax.rem(q + 2 * Z, Z)
            return full[slot, c, q].astype(F32) + pbuf[pb, q].astype(F32)

        if what == "give":
            swap.start()
        elif what == "on":
            if s:
                onwards(s - 1).wait_recv()
                onwards(s - 1).wait_send()
            else:
                swap.wait_recv()
                swap.wait_send()
            total = own(p + UP - s)
            on[r, s] = (total + on[r, s].astype(F32) if s else total).astype(BF)
            onwards(s).start()
        elif what == "back":
            if s:
                backwards(s - 1).wait_recv()
                backwards(s - 1).wait_send()
            total = own(p - DOWN + s)
            back[r, s] = (total + back[r, s].astype(F32) if s else total).astype(BF)
            backwards(s).start()
        else:
            for copy in (onwards(UP - 1), backwards(DOWN - 1)):
                copy.wait_recv()
                copy.wait_send()
            total = (own(p) + on[r, UP].astype(F32) + back[r, DOWN].astype(F32)).astype(BF)
            for k, out in enumerate(outs):

                @pl.when(lax.div(j, NT) == k)
                def _():
                    out[lax.rem(j, NT)] = total

    events = [(GIVE, "give", 0)] + [(STEPS + STRIDE * (s + 1), "on", s) for s in range(UP)] + [(STEPS + STRIDE * (s + 1) + LAG, "back", s) for s in range(DOWN)]
    events.append((STEPS + STRIDE * (UP + 1), "end", 0))

    def macro(i, _):
        for w in range(STEPS):

            @pl.when(i < J)
            def _():
                piece(i, w)

            for wait, what, s in sorted(events, reverse=True):
                if wait % STEPS == w:
                    j = i - wait // STEPS

                    @pl.when((j >= 0) & (j < J))
                    def _():
                        event(j, what, s)

        return 0

    lax.fori_loop(0, J + max(events)[0] // STEPS, macro, 0)


def grads(n, x, dy, wg, wu, wd):
    layers, D, FF = wg.shape
    T = x.shape[1]
    Z, HT, NT = n // 2, TILE // 2, FF // TILE
    R = (2 * HT // LANES) * (D // Z) + (D // LANES) * (HT // Z)
    dma, vmem, anywhere = pltpu.SemaphoreType.DMA, pltpu.VMEM, pl.BlockSpec(memory_space=pl.ANY)
    return pl.pallas_call(
        functools.partial(grads_kernel, n, layers),
        out_shape=[jax.ShapeDtypeStruct((NT, R, LANES), BF)] * layers,
        in_specs=[anywhere] * 5,
        out_specs=[pl.BlockSpec(memory_space=pltpu.VMEM)] * layers,
        scratch_shapes=[
            vmem((layers, T, D), BF),
            vmem((layers, T, D), BF),
            vmem((layers, T, D), BF),
            vmem((T, D), F32),
            vmem((2, D, TILE), BF),
            vmem((2, D, TILE), BF),
            vmem((2, TILE, D), BF),
            vmem((T, TILE), BF),
            vmem((T, TILE), BF),
            vmem((T, TILE), BF),
            vmem((NS, 2, Z, R, LANES), BF),
            vmem((NP, Z, R, LANES), BF),
            vmem((NR, Z // 2 + 1, R, LANES), BF),
            vmem((NR, Z - Z // 2, R, LANES), BF),
            dma((2,)),
            dma((2, 2, 3)),
            dma((NP,)),
            dma((NP,)),
            dma((NR,)),
            dma((NR, Z // 2 + 1)),
            dma((NR,)),
            dma((NR, Z - Z // 2)),
        ],
        compiler_params=pltpu.CompilerParams(collective_id=0, has_side_effects=True, vmem_limit_bytes=53 << 20),
        cost_estimate=pl.CostEstimate(flops=2 * T * D * FF * (11 * layers - 5), bytes_accessed=64 << 20, transcendentals=0),
        name="grads",
    )(x, dy, wg, wu, wd)


def adamw(w, m, v, g):
    m = 0.9 * m + 0.1 * g
    v = 0.95 * v + 0.05 * g * g
    step = m * lax.rsqrt(v + 1e-8) + 0.1 * w
    return (w - 0.02 * step).astype(BF), m, v


def update_kernel(n, l, s, sides, fetch, unread, *refs):
    terms, refs = refs[: len(sides)], refs[len(sides) :]
    olds, refs = refs[:9], refs[9 + unread :]
    news, (g, *bufs), (g_sem, in_sem, out_sem) = refs[:9], refs[9:19], refs[19:]
    at = Ring(n)
    Z = at.Z
    NT, _, _ = terms[0].shape
    D, FF = olds[0].shape[1:]
    HT = TILE // 2
    DR, FR = D // Z, HT // Z
    GC, DC = HT // LANES, D // LANES
    units, tiles = len(sides) * PARTS, NT // PARTS
    CW = tiles * HT

    def place(arrays, unit):
        side, part = (lax.div(unit, PARTS) if len(sides) > 1 else sides[0]), lax.rem(unit, PARTS)
        q = lax.rem(jnp.where(side == 0, at.p, at.mate_p) + (Z - s), Z)
        half = jnp.where(side == 0, at.c, 1 - at.c)
        rows = pl.ds(pl.multiple_of(q * DR, DR), DR)
        cols = pl.ds(pl.multiple_of(half * (FF // 2) + part * CW, CW), CW)
        return [x.at[l, rows, cols] for x in arrays[:6]] + [x.at[l, half, pl.ds(part * tiles, tiles), q] for x in arrays[6:]]

    def loads(unit):
        return [pltpu.make_async_copy(src, buf.at[unit], in_sem.at[unit, k]) for k, (src, buf) in enumerate(zip(place(olds, unit), bufs, strict=True))]

    def stores(unit):
        return [pltpu.make_async_copy(buf.at[unit], dst, out_sem.at[unit, k]) for k, (dst, buf) in enumerate(zip(place(news, unit), bufs, strict=True))]

    fetched = [pltpu.make_async_copy(terms[0].at[k], g.at[k], g_sem.at[k]) for k in range(NT if fetch else 0)]
    for unit in range(min(AHEAD, units)):
        for copy in (fetched[unit * tiles : (unit + 1) * tiles]) + loads(unit):
            copy.start()

    def one(unit, _):
        for k in range(len(fetched) // tiles):

            @pl.when(unit == k)
            def _():
                for copy in fetched[k * tiles : (k + 1) * tiles]:
                    copy.wait()

        for copy in loads(unit):
            copy.wait()

        @pl.when(unit + AHEAD < units)
        def _():
            for copy in loads(unit + AHEAD):
                copy.start()

        side, part = lax.div(unit, PARTS), lax.rem(unit, PARTS)

        def tile(t, _):
            def step(which, block, index):
                shards = [g, *terms[1:]] if fetch else terms
                grad = shards[0][part * tiles + t, block, :]
                if len(sides) > 1:
                    grad = jnp.where(side == 0, grad, shards[1][part * tiles + t, block, :])
                grad = grad.astype(F32)
                w, m, v = (bufs[3 * which + k] for k in range(3))
                w[index], m[index], v[index] = adamw(w[index].astype(F32), m[index], v[index], grad)

            for which in range(2):
                for k in range(GC):
                    cols = pl.ds(pl.multiple_of(t * HT + k * LANES, LANES), LANES)
                    step(which, pl.ds((which * GC + k) * DR, DR), (unit, slice(None), cols))
            for k in range(DC):
                step(2, pl.ds(2 * GC * DR + k * FR, FR), (unit, t, slice(None), pl.ds(k * LANES, LANES)))
            return 0

        lax.fori_loop(0, tiles, tile, 0)
        for copy in stores(unit):
            copy.start()
        return 0

    lax.fori_loop(0, units, one, 0)

    def end(unit, _):
        for copy in stores(unit):
            copy.wait()
        return 0

    lax.fori_loop(0, units, end, 0)


def update(n, l, s, terms, olds, news):
    sides, terms = tuple(terms), tuple(terms.values())
    fetch = sides[0] == 0 and 0 < s < n // 2 - 1
    NT, R, _ = terms[0].shape
    D, FF = olds[0].shape[1:]
    Z = n // 2
    dma, vmem, anywhere = pltpu.SemaphoreType.DMA, pltpu.VMEM, pl.BlockSpec(memory_space=pl.ANY)
    again = news is not None
    units, size = len(sides) * PARTS, len(sides) * terms[0].size
    wide, tall = (units, D // Z, FF // (2 * PARTS)), (units, NT // PARTS, TILE // 2 // Z, D)
    types = [BF, F32, F32]
    return pl.pallas_call(
        functools.partial(update_kernel, n, l, s, sides, fetch, 9 * again),
        out_shape=[jax.ShapeDtypeStruct(x.shape, x.dtype) for x in olds],
        in_specs=[anywhere if fetch and x == 0 else pl.BlockSpec(memory_space=vmem) for x in sides] + [anywhere] * (9 * (2 if again else 1)),
        out_specs=[anywhere] * 9,
        input_output_aliases={len(sides) + 9 + k: k for k in range(9)} if again else {},
        scratch_shapes=[vmem((NT, R, LANES), BF)]
        + [vmem(wide, t) for t in types] * 2
        + [vmem(tall, t) for t in types]
        + [dma((NT,)), dma((units, 9)), dma((units, 9))],
        compiler_params=pltpu.CompilerParams(vmem_limit_bytes=30 << 20),
        cost_estimate=pl.CostEstimate(flops=4 * 10**9 * len(sides), bytes_accessed=22 * size, transcendentals=size),
        name="update",
    )(*terms, *olds, *(news or ()))


def solution(mesh):
    n = mesh.shape["dp"]
    Z = n // 2
    onward = [(2 * z + c, 2 * ((z + 2 * c - 1) % Z) + c) for z in range(Z) for c in range(2)]
    across = [(2 * z + c, 2 * z + 1 - c) for z in range(Z) for c in range(2)]

    def step(x, dy, *arrays):
        weights, m, v = (arrays[i : i + 3] for i in (0, 3, 6))
        layers, D, FF = weights[0].shape
        NT = FF // TILE
        HT = TILE // 2
        terms = list(grads(n, x, dy, *weights))
        split = (layers, 2, NT, Z, HT // Z, D)
        olds = [y for w in range(3) for y in (weights[w], m[w], v[w])]
        shapes = [y.shape for y in olds]
        olds = olds[:6] + [y.reshape(split) for y in olds[6:]]

        def hop(k):
            return lax.ppermute(terms[k], "dp", onward)

        def swap(k):
            return lax.ppermute(terms[k], "dp", across)

        coming = [hop(k) for k in range(layers)]
        mates = [swap(k) for k in range(layers)]
        news = None
        for s in range(Z):
            for k in range(layers):
                shards = [{0: terms[k], 1: mates[k]}]
                if (k, s) == (layers - 1, Z - 1):
                    shards = [{0: terms[k]}, {1: mates[k]}]
                for part in shards:
                    news = update(n, layers - 1 - k, s, part, olds, news)
                if s < Z - 1:
                    terms[k] = coming[k]
                    if s < Z - 2:
                        coming[k] = hop(k)
                    mates[k] = swap(k)
        news = [y.reshape(shape) for y, shape in zip(news, shapes, strict=True)]
        return tuple(news[3 * w + which] for which in range(3) for w in range(3))

    return jax.shard_map(
        step,
        mesh=mesh,
        in_specs=(P(("rep", "dp"), None, None),) * 2 + (P(None, None, None),) * 9,
        out_specs=(P("rep", None, None),) * 9,
        check_vma=False,
    )
```
